32 devices in a mesh: mem: 8 (over z, y), hz: 4 (over x, core).
Axes of the slice: x: 2, y: 2, z: 4, core: 2. Of those that a mesh axis runs over, the one named last changes fastest.
Arguments:
- prior: float32 [8, 64, 32768], P('mem', None, 'hz'), may hold values from -6 to 6
- posterior: float32 [8, 64, 32768], P('mem', None, 'hz'), may hold values from -4 to 4
- control: float32 [64, 32768], P(None, 'hz'), may hold values from -6 to 6
- relax: float32 [64], replicated, may hold values from 0.5 to 0.95
- ocean: int32 [32768], P('hz'), may hold values 0 or 1
Outputs:
- analysis: float32 [8, 64, 32768], P('mem', None, 'hz')
The draws below stay inside these ranges and needn't reach their ends.
All inputs are finite; a program needn't handle non-finite values. No bound on the sum of `ocean` on one device may be relied on, other than what follows from the above.
Results may differ from the reference program's by a relative error of at most 0.00002.
Values sent between devices are 32-bit elements; how exact they have to be, the bound alone decides.
A program may use at most 64 MiB of HBM per device.

```python
import jax
import jax.numpy as jnp
from jax import lax

LEV = 64
MEMBERS = 8
NCOL = 32768


def touch_ends(drawn, rng, low, largest):
    dims = drawn.shape
    spot = [jax.random.randint(jax.random.fold_in(rng, axis), (), 0, dims[axis]) for axis in range(len(dims))]
    drawn = drawn.at[tuple(spot)].set(low)
    longest = dims.index(max(dims))
    spot[longest] = (spot[longest] + 1) % dims[longest]
    return drawn.at[tuple(spot)].set(largest)


def block_scale(key, shape, cuts, low, largest):
    def one(position, parts):
        draws = jax.random.uniform(jax.random.fold_in(jax.random.fold_in(key, 6), position), (parts,), jnp.float32, low / len(cuts), largest / len(cuts))
        return jnp.repeat(jnp.exp(draws), shape[position] // parts).reshape((-1,) + (1,) * (len(shape) - position - 1))

    loudness = one(*cuts[0])
    for cut in cuts[1:]:
        loudness = loudness * one(*cut)
    return loudness


def centred(key, dims, width, reach, shards=(), held_as=jnp.bfloat16):
    array = width * jax.random.normal(key, dims, jnp.float32)
    if shards:
        array = array * block_scale(key, dims, shards, -0.22, 0.18)
    return jnp.clip(array, -reach, reach).astype(held_as)


def setup_inputs(seed: int = 0) -> dict:
    key_of = jax.random.split(jax.random.key(seed), 6)
    prior = centred(key_of[0], (MEMBERS, LEV, NCOL), 1.0, 6.0, ((0, 8), (2, 4)), jnp.float32)
    posterior = centred(key_of[1], (MEMBERS, LEV, NCOL), 0.6, 4.0, ((0, 8), (2, 4)), jnp.float32)
    control = centred(key_of[2], (LEV, NCOL), 1.0, 6.0, ((1, 4),), jnp.float32)
    relax = jnp.clip(jax.random.uniform(key_of[3], (LEV,), jnp.float32, 0.5, 0.95), 0.5, 0.95)
    ocean = touch_ends((jax.random.randint(key_of[4], (NCOL,), 0, 4) < 3).astype(jnp.int32), jax.random.fold_in(key_of[4], 1), 0, 1)
    return {"prior": prior, "posterior": posterior, "control": control, "relax": relax, "ocean": ocean}


eps = 1e-06

def reference(prior, posterior, control, relax, ocean):
    prior_mean = lax.optimization_barrier(jnp.sum(prior, axis=0)) / MEMBERS
    post_mean = lax.optimization_barrier(jnp.sum(posterior, axis=0)) / MEMBERS
    weights = ocean.astype(jnp.float32)
    prior_anom = prior - prior_mean
    post_anom = posterior - post_mean
    prior_spread = lax.optimization_barrier(jnp.sum(prior_anom * prior_anom * weights, axis=(0, 2)))
    post_spread = lax.optimization_barrier(jnp.sum(post_anom * post_anom * weights, axis=(0, 2)))
    factor = relax * (jnp.sqrt((prior_spread + eps) / (post_spread + eps)) - 1.0) + 1.0
    return control + factor[None, :, None] * post_anom
```

```python
import functools

import jax
import jax.numpy as jnp
from jax import lax
from jax.experimental import pallas as pl
from jax.experimental.pallas import tpu as pltpu
from jax.sharding import PartitionSpec as P

eps = 1e-06
SUB = 8
LANE = 128
LAG = 2
MESH = pl.DeviceIdType.MESH
POST, PRIOR = 0, 1


def kernel(members, blocks, prior_hbm, post_hbm, control_hbm, relax_ref, ocean_ref, out_hbm,
           x, control, weights, total, out, y_in, pair, a_in, b_in, b_sum, b_swap, b_swap_prior, spread, part1, part2, zero,
           load_sem, control_sem, out_sem, y_send, y_recv, a_send, a_recv, b_send, b_recv, s_send, s_recv, p_send, p_recv,
           ga_send, ga_recv, gy_send, gy_recv, gb_send, gb_recv, h_send, h_recv, m_send, m_recv):
    levels, columns = control.shape
    half = columns // 2
    nblocks = levels // SUB
    quarter = nblocks // 4
    depth = members // 2
    m = lax.axis_index("mem")
    hz = lax.axis_index("hz")
    z = lax.div(m, 2)
    y = lax.rem(m, 2)
    other = 1 - y

    def device(zz, yy):
        return {"mem": zz * 2 + yy, "hz": hz}

    def rows(block):
        return pl.ds(pl.multiple_of(block * SUB, SUB), SUB)

    def cols(h):
        return pl.ds(pl.multiple_of(h * half, LANE), half)

    fields = (post_hbm, prior_hbm)

    def load(field, block):
        at = pl.ds(block * SUB, SUB)
        return pltpu.make_async_copy(fields[field].at[0, at], x.at[field, at], load_sem.at[field, block])

    order = []
    for i in range(2 * quarter):
        order += [i, 2 * quarter + i]
    for field in (POST, PRIOR):
        for block in order:
            load(field, block).start()
    control_load = pltpu.make_async_copy(control_hbm, control, control_sem)
    control_load.start()

    barrier = pltpu.get_barrier_semaphore()
    for i in range(1, members):
        pl.semaphore_signal(barrier, inc=1, device_id={"mem": lax.rem(m + i, members), "hz": hz}, device_id_type=MESH)
    for i in range(1, blocks):
        pl.semaphore_signal(barrier, inc=1, device_id={"mem": m, "hz": lax.rem(hz + i, blocks)}, device_id_type=MESH)
    weights[...] = jnp.broadcast_to(ocean_ref[...].astype(jnp.float32), (SUB, columns))
    spread[...] = jnp.zeros_like(spread)
    pl.semaphore_wait(barrier, members - 1 + blocks - 1)

    pending = []

    def send(src, dst, send_sem, recv_sem, to, cond=None):
        copy = pltpu.make_async_remote_copy(src_ref=src, dst_ref=dst, send_sem=send_sem, recv_sem=recv_sem,
                                            device_id=to, device_id_type=MESH)
        if cond is None:
            copy.start()
        else:
            pl.when(cond)(copy.start)
        pending.append((cond, copy))

    def arrive(dst, send_sem, recv_sem):
        pltpu.make_async_remote_copy(src_ref=dst, dst_ref=dst, send_sem=send_sem, recv_sem=recv_sem,
                                     device_id=device(z, other), device_id_type=MESH).wait_recv()

    def merge(own, n_own, came, n_came, dst, field, block, h, scale=None):
        n_own = jnp.float32(n_own)
        n_came = jnp.float32(n_came) if isinstance(n_came, int) else n_came.astype(jnp.float32)
        w = weights.at[:, cols(h)]
        acc = jnp.zeros((SUB, LANE), jnp.float32)
        for j in range(half // LANE):
            at = slice(j * LANE, (j + 1) * LANE)
            a, b = own[:, at], came[:, at]
            d = b * n_own - a * n_came
            acc += d * d * w[:, at]
            if dst is not None:
                dst[:, at] = a + b
        acc = acc / jnp.full((SUB, LANE), n_own * n_came * (n_own + n_came), jnp.float32)
        if scale is not None:
            acc = acc * scale
        spread[field, block] += acc

    up_near = 2 * z < depth
    near = jnp.where(up_near, 0, 1)
    far = 1 - near

    def place(d):
        at = jnp.where(d == 0, z, depth - 1 - z)
        return at, z + 1 - 2 * d, z - 1 + 2 * d

    def first(field):
        for i in range(2 * quarter):
            load(field, i).wait()
            send(x.at[field, pl.ds(i * SUB, SUB), cols(other)], y_in.at[field, i], y_send.at[field, i], y_recv.at[field, i],
                 device(z, other))
            load(field, 2 * quarter + i).wait()
        for k in range(quarter):
            for h in range(2):
                for d in (0, 1):
                    at, nxt, _ = place(d)
                    i = d * quarter + k
                    send(x.at[field, pl.ds((2 * quarter + i) * SUB, SUB), pl.ds(h * half, half)], b_in.at[field, i, h],
                         b_send.at[field, i, h], b_recv.at[field, i, h], device(nxt, y), (at == 0) & (at < depth - 1))

    def pair_step(field, i):
        arrive(y_in.at[field, i], y_send.at[field, i], y_recv.at[field, i])
        merge(x.at[field, pl.ds(i * SUB, SUB), cols(y)], 1, y_in.at[field, i], 1, pair.at[field, i], field, i, y)

    def a_step(field, d, k):
        at, nxt, back = place(d)
        i = d * quarter + k
        mine = pair.at[field, i]

        @pl.when(at > 0)
        def _():
            arrive(a_in.at[field, i], a_send.at[field, i], a_recv.at[field, i])
            merge(mine, 2, a_in.at[field, i], 2 * at, mine, field, i, y)

        send(mine, a_in.at[field, i], a_send.at[field, i], a_recv.at[field, i], device(nxt, y), at < depth - 1)
        if field == POST:
            last = at == depth - 1
            spot = total.at[rows(i), cols(y)]

            @pl.when(last)
            def _():
                spot[...] = mine[...]

            send(mine, spot, ga_send.at[i], ga_recv.at[i], device(back, y), last & (at > 0))
            send(mine, spot, gy_send.at[i], gy_recv.at[i], device(z, other), last)

    def b_step(field, d, k, h):
        at, nxt, _ = place(d)
        i = d * quarter + k
        block = 2 * quarter + i
        own = x.at[field, rows(block), cols(h)]
        mine = b_sum.at[field, i, h]

        @pl.when(at > 0)
        def _():
            arrive(b_in.at[field, i, h], b_send.at[field, i, h], b_recv.at[field, i, h])
            merge(own, 1, b_in.at[field, i, h], at, mine, field, block, h)

        last = at == depth - 1
        send(mine, b_in.at[field, i, h], b_send.at[field, i, h], b_recv.at[field, i, h], device(nxt, y), (at > 0) & ~last)
        if field == POST:
            send(mine, b_swap.at[i, h], s_send.at[i, h], s_recv.at[i, h], device(z, other), last)
        else:
            send(mine, b_swap_prior.at[i], p_send.at[i], p_recv.at[i], device(z, other), last & (other == h))

    def swap_step(d, k, h):
        at, _, back = place(d)
        i = d * quarter + k
        block = 2 * quarter + i
        last = at == depth - 1
        spot = total.at[rows(block), pl.ds(h * half, half)]

        @pl.when(last)
        def _():
            arrive(b_swap.at[i, h], s_send.at[i, h], s_recv.at[i, h])
            merge(b_sum.at[POST, i, h], depth, b_swap.at[i, h], depth, spot, POST, block, h, jnp.where(y == h, 1.0, 0.0))

        send(spot, spot, gb_send.at[i, h], gb_recv.at[i, h], device(back, y), last & (at > 0))

    def swap_prior(d, k):
        at, _, _ = place(d)
        i = d * quarter + k

        @pl.when(at == depth - 1)
        def _():
            arrive(b_swap_prior.at[i], p_send.at[i], p_recv.at[i])
            merge(b_sum.at[PRIOR, i, y], depth, b_swap_prior.at[i], depth, None, PRIOR, 2 * quarter + i, y)

    def a_relay(d, k):
        at, _, back = place(d)
        i = d * quarter + k
        spot = total.at[rows(i), cols(y)]
        below = at < depth - 1

        @pl.when(below)
        def _():
            arrive(spot, ga_send.at[i], ga_recv.at[i])

        send(spot, spot, ga_send.at[i], ga_recv.at[i], device(back, y), below & (at > 0))
        send(spot, spot, gy_send.at[i], gy_recv.at[i], device(z, other), below)

    def b_relay(d, k, h):
        at, _, back = place(d)
        i = d * quarter + k
        spot = total.at[rows(2 * quarter + i), pl.ds(h * half, half)]
        below = at < depth - 1

        @pl.when(below)
        def _():
            arrive(spot, gb_send.at[i, h], gb_recv.at[i, h])

        send(spot, spot, gb_send.at[i, h], gb_recv.at[i, h], device(back, y), below & (at > 0))

    first(POST)
    first(PRIOR)

    def chain(field):
        steps = []
        for k in range(quarter):
            for h in range(2):
                steps.append(functools.partial(lambda k, h, d: b_step(field, d, k, h), k, h))
        for k in range(quarter):
            steps.append(functools.partial(lambda k, d: a_step(field, d, k), k))
        return steps

    post_steps, prior_steps = chain(POST), chain(PRIOR)
    nb = 2 * quarter
    pairs = [(POST, i) for i in range(2 * quarter)] + [(PRIOR, i) for i in range(2 * quarter)]
    swaps = [functools.partial(lambda k, h, d: swap_step(d, k, h), k, h) for k in range(quarter) for h in range(2)]
    steps = post_steps + prior_steps
    n = len(steps)
    done_pairs = 0
    for s in range(n + LAG):
        if done_pairs < len(pairs):
            pair_step(*pairs[done_pairs])
            done_pairs += 1
        if s < n:
            steps[s](near)
        if s >= LAG:
            steps[s - LAG](far)
        t = s - LAG - nb
        if 0 <= t < len(swaps):
            swaps[t](0)
            swaps[t](1)
    for k in range(quarter):
        swap_prior(0, k)
        swap_prior(1, k)

    lane = lax.broadcasted_iota(jnp.int32, (SUB, LANE), 1)
    for field in (POST, PRIOR):
        packed = jnp.zeros((SUB, LANE), jnp.float32)
        for block in range(nblocks):
            packed = jnp.where(lane == block, jnp.sum(spread[field, block], axis=1, keepdims=True), packed)
        part1[hz, field] = packed
    for i in range(1, blocks):
        send(part1.at[hz], part1.at[hz], h_send.at[i], h_recv.at[hz], {"mem": m, "hz": lax.rem(hz + i, blocks)})

    units = [(None, k) for k in range(quarter)] + [(h, k) for k in range(quarter) for h in range(2)]

    def relay(d, h, k):
        if h is None:
            a_relay(d, k)
        else:
            b_relay(d, k, h)

    events = []
    for s in range(len(units) + 1):
        if s < len(units):
            events.append((far, *units[s]))
        if s >= 1:
            events.append((near, *units[s - 1]))
    cut1, cut2 = len(events) // 3, 2 * len(events) // 3
    for event in events[:cut1]:
        relay(*event)
    for i in range(1, blocks):
        src = lax.rem(hz + i, blocks)
        arrive(part1.at[src], h_send.at[i], h_recv.at[src])
    for field in (POST, PRIOR):
        v = part1[0, field]
        for i in range(1, blocks):
            v = v + part1[i, field]
        part2[m, field] = v
    for i in range(1, members):
        send(part2.at[m], part2.at[m], m_send.at[i], m_recv.at[m], {"mem": lax.rem(m + i, members), "hz": hz})
    for event in events[cut1:cut2]:
        relay(*event)
    for i in range(1, members):
        src = lax.rem(m + i, members)
        arrive(part2.at[src], m_send.at[i], m_recv.at[src])
    spreads = []
    for field in (POST, PRIOR):
        v = part2[0, field]
        for i in range(1, members):
            v = v + part2[i, field]
        spreads.append(v)
    sub = lax.broadcasted_iota(jnp.int32, (SUB, LANE), 0)
    relax = jnp.zeros((SUB, LANE), jnp.float32)
    for level in range(levels):
        relax = jnp.where((sub == level % SUB) & (lane == level // SUB), relax_ref[level], relax)
    factor = relax * (jnp.sqrt((spreads[PRIOR] + eps) / (spreads[POST] + eps)) - 1.0) + 1.0
    for block in range(nblocks):
        zero[block] = jnp.broadcast_to(
            jnp.sum(jnp.where(lane == block, factor, 0.0), axis=1, keepdims=True), (SUB, LANE))
    control_load.wait()

    outs = []

    def finish(block, h):
        f = zero[block]
        c, p, t, o = (r.at[rows(block), cols(h)] for r in (control, x.at[POST], total, out))
        for j in range(half // LANE):
            at = slice(j * LANE, (j + 1) * LANE)
            o[:, at] = c[:, at] + f * (p[:, at] - t[:, at] / members)
        copy = pltpu.make_async_copy(o, out_hbm.at[0, rows(block), cols(h)], out_sem.at[block, h])
        copy.start()
        outs.append(copy)

    for i, (d, h, k) in enumerate(events):
        if i >= cut2:
            relay(d, h, k)
        if h is None:
            finish(d * quarter + k, y)
        else:
            finish(2 * quarter + d * quarter + k, h)
    for k in range(quarter):
        for d in (near, far):
            i = d * quarter + k
            arrive(total.at[rows(i), cols(other)], gy_send.at[i], gy_recv.at[i])
            finish(i, other)
    for cond, copy in pending:
        if cond is None:
            copy.wait_send()
        else:
            pl.when(cond)(copy.wait_send)
    for copy in outs:
        copy.wait()


def solution(mesh):
    members, blocks = mesh.shape["mem"], mesh.shape["hz"]

    def on_device(prior, posterior, control, relax, ocean):
        levels, columns = control.shape
        half, nblocks = columns // 2, levels // SUB
        a, q = nblocks // 2, nblocks // 4
        vmem = lambda *shape: pltpu.VMEM(shape, jnp.float32)
        dma = lambda *shape: pltpu.SemaphoreType.DMA(shape)
        hbm = pl.BlockSpec(memory_space=pl.ANY)
        return pl.pallas_call(
            functools.partial(kernel, members, blocks),
            out_shape=jax.ShapeDtypeStruct(posterior.shape, jnp.float32),
            in_specs=[hbm, hbm, hbm, pl.BlockSpec(memory_space=pltpu.SMEM), pl.BlockSpec(memory_space=pltpu.VMEM)],
            out_specs=hbm,
            scratch_shapes=[
                vmem(2, levels, columns), vmem(levels, columns), vmem(SUB, columns), vmem(levels, columns),
                vmem(levels, columns), vmem(2, a, SUB, half), vmem(2, a, SUB, half), vmem(2, a, SUB, half),
                vmem(2, a, 2, SUB, half), vmem(2, a, 2, SUB, half), vmem(a, 2, SUB, half), vmem(a, SUB, half),
                vmem(2, nblocks, SUB, LANE), vmem(blocks, 2, SUB, LANE), vmem(members, 2, SUB, LANE),
                vmem(nblocks, SUB, LANE),
                dma(2, nblocks), pltpu.SemaphoreType.DMA, dma(nblocks, 2),
                dma(2, a), dma(2, a), dma(2, a), dma(2, a), dma(2, a, 2), dma(2, a, 2), dma(a, 2), dma(a, 2), dma(a), dma(a),
                dma(a), dma(a), dma(a), dma(a), dma(a, 2), dma(a, 2), dma(blocks), dma(blocks), dma(members), dma(members),
            ],
            compiler_params=pltpu.CompilerParams(
                collective_id=0, has_side_effects=True, vmem_limit_bytes=60 * 2**20
            ),
        )(prior, posterior, control, relax, ocean.reshape(1, columns))

    return jax.shard_map(
        on_device,
        mesh=mesh,
        in_specs=(P("mem", None, "hz"), P("mem", None, "hz"), P(None, "hz"), P(), P("hz")),
        out_specs=P("mem", None, "hz"),
        check_vma=False,
    )
```

```python
import functools

import jax
import jax.numpy as jnp
from jax import lax
from jax.experimental import pallas as pl
from jax.experimental.pallas import tpu as pltpu
from jax.sharding import PartitionSpec as P

eps = 1e-06
SUB = 8
LANE = 128
LAG = 2
MESH = pl.DeviceIdType.MESH
POST, PRIOR = 0, 1


def kernel(members, blocks, prior_hbm, post_hbm, control_hbm, relax_ref, ocean_ref, out_hbm,
           x, control, weights, total, out, y_in, pair, a_in, b_in, b_sum, b_swap, b_swap_prior, spread, part1, part2, zero,
           load_sem, control_sem, out_sem, y_send, y_recv, a_send, a_recv, b_send, b_recv, s_send, s_recv, p_send, p_recv,
           ga_send, ga_recv, gy_send, gy_recv, gb_send, gb_recv, h_send, h_recv, m_send, m_recv):
    levels, columns = control.shape
    half = columns // 2
    nblocks = levels // SUB
    quarter = nblocks // 4
    depth = members // 2
    m = lax.axis_index("mem")
    hz = lax.axis_index("hz")
    z = lax.div(m, 2)
    y = lax.rem(m, 2)
    other = 1 - y

    def device(zz, yy):
        return {"mem": zz * 2 + yy, "hz": hz}

    def rows(block):
        return pl.ds(pl.multiple_of(block * SUB, SUB), SUB)

    def cols(h):
        return pl.ds(pl.multiple_of(h * half, LANE), half)

    fields = (post_hbm, prior_hbm)

    def load(field, block):
        at = pl.ds(block * SUB, SUB)
        return pltpu.make_async_copy(fields[field].at[0, at], x.at[field, at], load_sem.at[field, block])

    order = []
    for i in range(2 * quarter):
        order += [i, 2 * quarter + i]
    for field in (POST, PRIOR):
        for block in order:
            load(field, block).start()
    control_load = pltpu.make_async_copy(control_hbm, control, control_sem)
    control_load.start()

    barrier = pltpu.get_barrier_semaphore()
    for i in range(1, members):
        pl.semaphore_signal(barrier, inc=1, device_id={"mem": lax.rem(m + i, members), "hz": hz}, device_id_type=MESH)
    for i in range(1, blocks):
        pl.semaphore_signal(barrier, inc=1, device_id={"mem": m, "hz": lax.rem(hz + i, blocks)}, device_id_type=MESH)
    weights[...] = jnp.broadcast_to(ocean_ref[...].astype(jnp.float32), (SUB, columns))
    spread[...] = jnp.zeros_like(spread)
    pl.semaphore_wait(barrier, members - 1 + blocks - 1)

    pending = []

    def send(src, dst, send_sem, recv_sem, to, cond=None):
        copy = pltpu.make_async_remote_copy(src_ref=src, dst_ref=dst, send_sem=send_sem, recv_sem=recv_sem,
                                            device_id=to, device_id_type=MESH)
        if cond is None:
            copy.start()
        else:
            pl.when(cond)(copy.start)
        pending.append((cond, copy))

    def arrive(dst, send_sem, recv_sem):
        pltpu.make_async_remote_copy(src_ref=dst, dst_ref=dst, send_sem=send_sem, recv_sem=recv_sem,
                                     device_id=device(z, other), device_id_type=MESH).wait_recv()

    def merge(own, n_own, came, n_came, dst, field, block, h, scale=None):
        n_own = jnp.float32(n_own)
        n_came = jnp.float32(n_came) if isinstance(n_came, int) else n_came.astype(jnp.float32)
        w = weights.at[:, cols(h)]
        acc = jnp.zeros((SUB, LANE), jnp.float32)
        for j in range(half // LANE):
            at = slice(j * LANE, (j + 1) * LANE)
            a, b = own[:, at], came[:, at]
            d = b * n_own - a * n_came
            acc += d * d * w[:, at]
            if dst is not None:
                dst[:, at] = a + b
        acc = acc / jnp.full((SUB, LANE), n_own * n_came * (n_own + n_came), jnp.float32)
        if scale is not None:
            acc = acc * scale
        spread[field, block] += acc

    up_near = 2 * z < depth
    near = jnp.where(up_near, 0, 1)
    far = 1 - near

    def place(d):
        at = jnp.where(d == 0, z, depth - 1 - z)
        return at, z + 1 - 2 * d, z - 1 + 2 * d

    def first(field):
        for block in order:
            load(field, block).wait()
        for d in (near, far):
            for k in range(quarter):
                i = d * quarter + k
                send(x.at[field, rows(i), cols(other)], y_in.at[field, i], y_send.at[field, i], y_recv.at[field, i],
                     device(z, other))

    def start_b(field):
        at, nxt, _ = place(near)
        for k in range(quarter):
            for h in range(2):
                i = near * quarter + k
                send(x.at[field, rows(2 * quarter + i), pl.ds(h * half, half)], b_in.at[field, i, h],
                     b_send.at[field, i, h], b_recv.at[field, i, h], device(nxt, y), (at == 0) & (at < depth - 1))

    def pair_step(field, d, k):
        at, nxt, _ = place(d)
        i = d * quarter + k
        mine = pair.at[field, i]
        arrive(y_in.at[field, i], y_send.at[field, i], y_recv.at[field, i])
        merge(x.at[field, rows(i), cols(y)], 1, y_in.at[field, i], 1, mine, field, i, y)
        send(mine, a_in.at[field, i], a_send.at[field, i], a_recv.at[field, i], device(nxt, y), (at == 0) & (at < depth - 1))

    def a_step(field, d, k):
        at, nxt, back = place(d)
        i = d * quarter + k
        mine = pair.at[field, i]

        @pl.when(at > 0)
        def _():
            arrive(a_in.at[field, i], a_send.at[field, i], a_recv.at[field, i])
            merge(mine, 2, a_in.at[field, i], 2 * at, mine, field, i, y)

        send(mine, a_in.at[field, i], a_send.at[field, i], a_recv.at[field, i], device(nxt, y), (at > 0) & (at < depth - 1))
        if field == POST:
            last = at == depth - 1
            spot = total.at[rows(i), cols(y)]

            @pl.when(last)
            def _():
                spot[...] = mine[...]

            send(mine, spot, ga_send.at[i], ga_recv.at[i], device(back, y), last & (at > 0))
            send(mine, spot, gy_send.at[i], gy_recv.at[i], device(z, other), last)

    def b_step(field, d, k, h):
        at, nxt, _ = place(d)
        i = d * quarter + k
        block = 2 * quarter + i
        own = x.at[field, rows(block), cols(h)]
        mine = b_sum.at[field, i, h]

        @pl.when(at > 0)
        def _():
            arrive(b_in.at[field, i, h], b_send.at[field, i, h], b_recv.at[field, i, h])
            merge(own, 1, b_in.at[field, i, h], at, mine, field, block, h)

        last = at == depth - 1
        send(mine, b_in.at[field, i, h], b_send.at[field, i, h], b_recv.at[field, i, h], device(nxt, y), (at > 0) & ~last)
        if field == POST:
            send(mine, b_swap.at[i, h], s_send.at[i, h], s_recv.at[i, h], device(z, other), last)
        else:
            send(mine, b_swap_prior.at[i], p_send.at[i], p_recv.at[i], device(z, other), last & (other == h))

    def swap_step(d, k, h):
        at, _, back = place(d)
        i = d * quarter + k
        block = 2 * quarter + i
        last = at == depth - 1
        spot = total.at[rows(block), pl.ds(h * half, half)]

        @pl.when(last)
        def _():
            arrive(b_swap.at[i, h], s_send.at[i, h], s_recv.at[i, h])
            merge(b_sum.at[POST, i, h], depth, b_swap.at[i, h], depth, spot, POST, block, h, jnp.where(y == h, 1.0, 0.0))

        send(spot, spot, gb_send.at[i, h], gb_recv.at[i, h], device(back, y), last & (at > 0))

    def swap_prior(d, k):
        at, _, _ = place(d)
        i = d * quarter + k

        @pl.when(at == depth - 1)
        def _():
            arrive(b_swap_prior.at[i], p_send.at[i], p_recv.at[i])
            merge(b_sum.at[PRIOR, i, y], depth, b_swap_prior.at[i], depth, None, PRIOR, 2 * quarter + i, y)

    def a_relay(d, k):
        at, _, back = place(d)
        i = d * quarter + k
        spot = total.at[rows(i), cols(y)]
        below = at < depth - 1

        @pl.when(below)
        def _():
            arrive(spot, ga_send.at[i], ga_recv.at[i])

        send(spot, spot, ga_send.at[i], ga_recv.at[i], device(back, y), below & (at > 0))
        send(spot, spot, gy_send.at[i], gy_recv.at[i], device(z, other), below)

    def b_relay(d, k, h):
        at, _, back = place(d)
        i = d * quarter + k
        spot = total.at[rows(2 * quarter + i), pl.ds(h * half, half)]
        below = at < depth - 1

        @pl.when(below)
        def _():
            arrive(spot, gb_send.at[i, h], gb_recv.at[i, h])

        send(spot, spot, gb_send.at[i, h], gb_recv.at[i, h], device(back, y), below & (at > 0))

    first(POST)
    start_b(POST)
    first(PRIOR)

    def chain(field):
        steps = []
        for k in range(quarter):
            for h in range(2):
                steps.append(functools.partial(lambda k, h, d: b_step(field, d, k, h), k, h))
        for k in range(quarter):
            steps.append(functools.partial(lambda k, d: a_step(field, d, k), k))
        return steps

    post_steps, prior_steps = chain(POST), chain(PRIOR)
    nb = 2 * quarter
    pairs = [(field, d, k) for field in (POST, PRIOR) for d in (near, far) for k in range(quarter)]
    swaps = [functools.partial(lambda k, h, d: swap_step(d, k, h), k, h) for k in range(quarter) for h in range(2)]
    steps = post_steps + prior_steps
    n = len(steps)
    done_pairs = 0
    for s in range(n + LAG):
        if done_pairs < len(pairs):
            pair_step(*pairs[done_pairs])
            done_pairs += 1
            if done_pairs == quarter:
                start_b(PRIOR)
        if s < n:
            steps[s](near)
        if s >= LAG:
            steps[s - LAG](far)
        t = s - LAG - nb - 1
        if 0 <= t < len(swaps):
            swaps[t](0)
            swaps[t](1)
    for k in range(quarter):
        swap_prior(0, k)
        swap_prior(1, k)

    lane = lax.broadcasted_iota(jnp.int32, (SUB, LANE), 1)
    for field in (POST, PRIOR):
        packed = jnp.zeros((SUB, LANE), jnp.float32)
        for block in range(nblocks):
            packed = jnp.where(lane == block, jnp.sum(spread[field, block], axis=1, keepdims=True), packed)
        part1[hz, field] = packed
    for i in range(1, blocks):
        send(part1.at[hz], part1.at[hz], h_send.at[i], h_recv.at[hz], {"mem": m, "hz": lax.rem(hz + i, blocks)})

    units = [(None, k) for k in range(quarter)] + [(h, k) for k in range(quarter) for h in range(2)]

    def relay(d, h, k):
        if h is None:
            a_relay(d, k)
        else:
            b_relay(d, k, h)

    events = []
    for s in range(len(units) + 1):
        if s < len(units):
            events.append((far, *units[s]))
        if s >= 1:
            events.append((near, *units[s - 1]))
    cut1, cut2 = len(events) // 3, 2 * len(events) // 3
    for event in events[:cut1]:
        relay(*event)
    for i in range(1, blocks):
        src = lax.rem(hz + i, blocks)
        arrive(part1.at[src], h_send.at[i], h_recv.at[src])
    for field in (POST, PRIOR):
        v = part1[0, field]
        for i in range(1, blocks):
            v = v + part1[i, field]
        part2[m, field] = v
    for i in range(1, members):
        send(part2.at[m], part2.at[m], m_send.at[i], m_recv.at[m], {"mem": lax.rem(m + i, members), "hz": hz})
    for event in events[cut1:cut2]:
        relay(*event)
    for i in range(1, members):
        src = lax.rem(m + i, members)
        arrive(part2.at[src], m_send.at[i], m_recv.at[src])
    spreads = []
    for field in (POST, PRIOR):
        v = part2[0, field]
        for i in range(1, members):
            v = v + part2[i, field]
        spreads.append(v)
    sub = lax.broadcasted_iota(jnp.int32, (SUB, LANE), 0)
    relax = jnp.zeros((SUB, LANE), jnp.float32)
    for level in range(levels):
        relax = jnp.where((sub == level % SUB) & (lane == level // SUB), relax_ref[level], relax)
    factor = relax * (jnp.sqrt((spreads[PRIOR] + eps) / (spreads[POST] + eps)) - 1.0) + 1.0
    for block in range(nblocks):
        zero[block] = jnp.broadcast_to(
            jnp.sum(jnp.where(lane == block, factor, 0.0), axis=1, keepdims=True), (SUB, LANE))
    control_load.wait()

    outs = []

    def finish(block, h):
        f = zero[block]
        c, p, t, o = (r.at[rows(block), cols(h)] for r in (control, x.at[POST], total, out))
        for j in range(half // LANE):
            at = slice(j * LANE, (j + 1) * LANE)
            o[:, at] = c[:, at] + f * (p[:, at] - t[:, at] / members)
        copy = pltpu.make_async_copy(o, out_hbm.at[0, rows(block), cols(h)], out_sem.at[block, h])
        copy.start()
        outs.append(copy)

    for i, (d, h, k) in enumerate(events):
        if i >= cut2:
            relay(d, h, k)
        if h is None:
            finish(d * quarter + k, y)
        else:
            finish(2 * quarter + d * quarter + k, h)
    for k in range(quarter):
        for d in (near, far):
            i = d * quarter + k
            arrive(total.at[rows(i), cols(other)], gy_send.at[i], gy_recv.at[i])
            finish(i, other)
    for cond, copy in pending:
        if cond is None:
            copy.wait_send()
        else:
            pl.when(cond)(copy.wait_send)
    for copy in outs:
        copy.wait()


def solution(mesh):
    members, blocks = mesh.shape["mem"], mesh.shape["hz"]

    def on_device(prior, posterior, control, relax, ocean):
        levels, columns = control.shape
        half, nblocks = columns // 2, levels // SUB
        a, q = nblocks // 2, nblocks // 4
        vmem = lambda *shape: pltpu.VMEM(shape, jnp.float32)
        dma = lambda *shape: pltpu.SemaphoreType.DMA(shape)
        hbm = pl.BlockSpec(memory_space=pl.ANY)
        return pl.pallas_call(
            functools.partial(kernel, members, blocks),
            out_shape=jax.ShapeDtypeStruct(posterior.shape, jnp.float32),
            in_specs=[hbm, hbm, hbm, pl.BlockSpec(memory_space=pltpu.SMEM), pl.BlockSpec(memory_space=pltpu.VMEM)],
            out_specs=hbm,
            scratch_shapes=[
                vmem(2, levels, columns), vmem(levels, columns), vmem(SUB, columns), vmem(levels, columns),
                vmem(levels, columns), vmem(2, a, SUB, half), vmem(2, a, SUB, half), vmem(2, a, SUB, half),
                vmem(2, a, 2, SUB, half), vmem(2, a, 2, SUB, half), vmem(a, 2, SUB, half), vmem(a, SUB, half),
                vmem(2, nblocks, SUB, LANE), vmem(blocks, 2, SUB, LANE), vmem(members, 2, SUB, LANE),
                vmem(nblocks, SUB, LANE),
                dma(2, nblocks), pltpu.SemaphoreType.DMA, dma(nblocks, 2),
                dma(2, a), dma(2, a), dma(2, a), dma(2, a), dma(2, a, 2), dma(2, a, 2), dma(a, 2), dma(a, 2), dma(a), dma(a),
                dma(a), dma(a), dma(a), dma(a), dma(a, 2), dma(a, 2), dma(blocks), dma(blocks), dma(members), dma(members),
            ],
            compiler_params=pltpu.CompilerParams(
                collective_id=0, has_side_effects=True, vmem_limit_bytes=60 * 2**20
            ),
        )(prior, posterior, control, relax, ocean.reshape(1, columns))

    return jax.shard_map(
        on_device,
        mesh=mesh,
        in_specs=(P("mem", None, "hz"), P("mem", None, "hz"), P(None, "hz"), P(), P("hz")),
        out_specs=P("mem", None, "hz"),
        check_vma=False,
    )
```

```python
import functools

import jax
import jax.numpy as jnp
from jax import lax
from jax.experimental import pallas as pl
from jax.experimental.pallas import tpu as pltpu
from jax.sharding import PartitionSpec as P

eps = 1e-06
SUB = 8
LANE = 128
LAG = 2
MESH = pl.DeviceIdType.MESH
POST, PRIOR = 0, 1


def kernel(members, blocks, prior_hbm, post_hbm, control_hbm, relax_ref, ocean_ref, out_hbm,
           x, control, weights, total, out, y_in, pair, a_in, b_in, b_sum, b_swap, b_swap_prior, spread, part1, part2, zero,
           load_sem, control_sem, out_sem, y_send, y_recv, a_send, a_recv, b_send, b_recv, s_send, s_recv, p_send, p_recv,
           ga_send, ga_recv, gy_send, gy_recv, gb_send, gb_recv, h_send, h_recv, m_send, m_recv):
    levels, columns = control.shape
    half = columns // 2
    nblocks = levels // SUB
    quarter = nblocks // 4
    depth = members // 2
    m = lax.axis_index("mem")
    hz = lax.axis_index("hz")
    z = lax.div(m, 2)
    y = lax.rem(m, 2)
    other = 1 - y

    def device(zz, yy):
        return {"mem": zz * 2 + yy, "hz": hz}

    def rows(block):
        return pl.ds(pl.multiple_of(block * SUB, SUB), SUB)

    def cols(h):
        return pl.ds(pl.multiple_of(h * half, LANE), half)

    fields = (post_hbm, prior_hbm)

    def load(field, block):
        at = pl.ds(block * SUB, SUB)
        return pltpu.make_async_copy(fields[field].at[0, at], x.at[field, at], load_sem.at[field, block])

    order = []
    for i in range(2 * quarter):
        order += [i, 2 * quarter + i]
    for field in (POST, PRIOR):
        for block in order:
            load(field, block).start()
    control_load = pltpu.make_async_copy(control_hbm, control, control_sem)
    control_load.start()

    barrier = pltpu.get_barrier_semaphore()
    for i in range(1, members):
        pl.semaphore_signal(barrier, inc=1, device_id={"mem": lax.rem(m + i, members), "hz": hz}, device_id_type=MESH)
    for i in range(1, blocks):
        pl.semaphore_signal(barrier, inc=1, device_id={"mem": m, "hz": lax.rem(hz + i, blocks)}, device_id_type=MESH)
    weights[...] = jnp.broadcast_to(ocean_ref[...].astype(jnp.float32), (SUB, columns))
    spread[...] = jnp.zeros_like(spread)
    pl.semaphore_wait(barrier, members - 1 + blocks - 1)

    pending = []

    def send(src, dst, send_sem, recv_sem, to, cond=None):
        copy = pltpu.make_async_remote_copy(src_ref=src, dst_ref=dst, send_sem=send_sem, recv_sem=recv_sem,
                                            device_id=to, device_id_type=MESH)
        if cond is None:
            copy.start()
        else:
            pl.when(cond)(copy.start)
        pending.append((cond, copy))

    def arrive(dst, send_sem, recv_sem):
        pltpu.make_async_remote_copy(src_ref=dst, dst_ref=dst, send_sem=send_sem, recv_sem=recv_sem,
                                     device_id=device(z, other), device_id_type=MESH).wait_recv()

    def merge(own, n_own, came, n_came, dst, field, block, h, scale=None):
        n_own = jnp.float32(n_own)
        n_came = jnp.float32(n_came) if isinstance(n_came, int) else n_came.astype(jnp.float32)
        w = weights.at[:, cols(h)]
        acc = jnp.zeros((SUB, LANE), jnp.float32)
        for j in range(half // LANE):
            at = slice(j * LANE, (j + 1) * LANE)
            a, b = own[:, at], came[:, at]
            d = b * n_own - a * n_came
            acc += d * d * w[:, at]
            if dst is not None:
                dst[:, at] = a + b
        acc = acc / jnp.full((SUB, LANE), n_own * n_came * (n_own + n_came), jnp.float32)
        if scale is not None:
            acc = acc * scale
        spread[field, block] += acc

    up_near = 2 * z < depth
    near = jnp.where(up_near, 0, 1)
    far = 1 - near

    def place(d):
        at = jnp.where(d == 0, z, depth - 1 - z)
        return at, z + 1 - 2 * d, z - 1 + 2 * d

    def first(field):
        for block in order:
            load(field, block).wait()
        for d in (near, far):
            for k in range(quarter):
                i = d * quarter + k
                send(x.at[field, rows(i), cols(other)], y_in.at[field, i], y_send.at[field, i], y_recv.at[field, i],
                     device(z, other))

    def start_b(field):
        at, nxt, _ = place(near)
        for k in range(quarter):
            for h in range(2):
                i = near * quarter + k
                send(x.at[field, rows(2 * quarter + i), pl.ds(h * half, half)], b_in.at[field, i, h],
                     b_send.at[field, i, h], b_recv.at[field, i, h], device(nxt, y), (at == 0) & (at < depth - 1))

    def pair_step(field, d, k):
        at, nxt, _ = place(d)
        i = d * quarter + k
        mine = pair.at[field, i]
        arrive(y_in.at[field, i], y_send.at[field, i], y_recv.at[field, i])
        merge(x.at[field, rows(i), cols(y)], 1, y_in.at[field, i], 1, mine, field, i, y)
        send(mine, a_in.at[field, i], a_send.at[field, i], a_recv.at[field, i], device(nxt, y), (at == 0) & (at < depth - 1))

    def a_step(field, d, k):
        at, nxt, back = place(d)
        i = d * quarter + k
        mine = pair.at[field, i]

        @pl.when(at > 0)
        def _():
            arrive(a_in.at[field, i], a_send.at[field, i], a_recv.at[field, i])
            merge(mine, 2, a_in.at[field, i], 2 * at, mine, field, i, y)

        send(mine, a_in.at[field, i], a_send.at[field, i], a_recv.at[field, i], device(nxt, y), (at > 0) & (at < depth - 1))
        if field == POST:
            last = at == depth - 1
            spot = total.at[rows(i), cols(y)]

            @pl.when(last)
            def _():
                spot[...] = mine[...]

            send(mine, spot, ga_send.at[i], ga_recv.at[i], device(back, y), last & (at > 0))
            send(mine, spot, gy_send.at[i], gy_recv.at[i], device(z, other), last)

    def b_step(field, d, k, h):
        at, nxt, _ = place(d)
        i = d * quarter + k
        block = 2 * quarter + i
        own = x.at[field, rows(block), cols(h)]
        mine = b_sum.at[field, i, h]

        @pl.when(at > 0)
        def _():
            arrive(b_in.at[field, i, h], b_send.at[field, i, h], b_recv.at[field, i, h])
            merge(own, 1, b_in.at[field, i, h], at, mine, field, block, h)

        last = at == depth - 1
        send(mine, b_in.at[field, i, h], b_send.at[field, i, h], b_recv.at[field, i, h], device(nxt, y), (at > 0) & ~last)
        if field == POST:
            send(mine, b_swap.at[i, h], s_send.at[i, h], s_recv.at[i, h], device(z, other), last)
        else:
            send(mine, b_swap_prior.at[i], p_send.at[i], p_recv.at[i], device(z, other), last & (other == h))

    def swap_step(d, k, h):
        at, _, back = place(d)
        i = d * quarter + k
        block = 2 * quarter + i
        last = at == depth - 1
        spot = total.at[rows(block), pl.ds(h * half, half)]

        @pl.when(last)
        def _():
            arrive(b_swap.at[i, h], s_send.at[i, h], s_recv.at[i, h])
            merge(b_sum.at[POST, i, h], depth, b_swap.at[i, h], depth, spot, POST, block, h, jnp.where(y == h, 1.0, 0.0))

        send(spot, spot, gb_send.at[i, h], gb_recv.at[i, h], device(back, y), last & (at > 0))

    def swap_prior(d, k):
        at, _, _ = place(d)
        i = d * quarter + k

        @pl.when(at == depth - 1)
        def _():
            arrive(b_swap_prior.at[i], p_send.at[i], p_recv.at[i])
            merge(b_sum.at[PRIOR, i, y], depth, b_swap_prior.at[i], depth, None, PRIOR, 2 * quarter + i, y)

    def a_relay(d, k):
        at, _, back = place(d)
        i = d * quarter + k
        spot = total.at[rows(i), cols(y)]
        below = at < depth - 1

        @pl.when(below)
        def _():
            arrive(spot, ga_send.at[i], ga_recv.at[i])

        send(spot, spot, ga_send.at[i], ga_recv.at[i], device(back, y), below & (at > 0))
        send(spot, spot, gy_send.at[i], gy_recv.at[i], device(z, other), below)

    def b_relay(d, k, h):
        at, _, back = place(d)
        i = d * quarter + k
        spot = total.at[rows(2 * quarter + i), pl.ds(h * half, half)]
        below = at < depth - 1

        @pl.when(below)
        def _():
            arrive(spot, gb_send.at[i, h], gb_recv.at[i, h])

        send(spot, spot, gb_send.at[i, h], gb_recv.at[i, h], device(back, y), below & (at > 0))

    first(POST)
    start_b(POST)
    first(PRIOR)

    def chain(field):
        steps = []
        for k in range(quarter):
            for h in range(2):
                steps.append(functools.partial(lambda k, h, d: b_step(field, d, k, h), k, h))
        for k in range(quarter):
            steps.append(functools.partial(lambda k, d: a_step(field, d, k), k))
        return steps

    post_steps, prior_steps = chain(POST), chain(PRIOR)
    nb = 2 * quarter
    pairs = [(field, d, k) for field in (POST, PRIOR) for d in (near, far) for k in range(quarter)]
    swaps = [functools.partial(lambda k, h, d: swap_step(d, k, h), k, h) for k in range(quarter) for h in range(2)]
    steps = post_steps + prior_steps
    n = len(steps)
    units = [(None, k) for k in range(quarter)] + [(h, k) for k in range(quarter) for h in range(2)]

    def relay(d, h, k):
        if h is None:
            a_relay(d, k)
        else:
            b_relay(d, k, h)

    events = []
    for u in range(len(units) + 1):
        if u < len(units):
            events.append((far, *units[u]))
        if u >= 1:
            events.append((near, *units[u - 1]))
    cut1, cut2 = len(events) // 3, 2 * len(events) // 3
    done_pairs = 0
    for s in range(n + LAG):
        if done_pairs < len(pairs):
            pair_step(*pairs[done_pairs])
            done_pairs += 1
            if done_pairs == quarter:
                start_b(PRIOR)
        if s < n:
            steps[s](near)
        if s >= LAG:
            steps[s - LAG](far)
        t = s - LAG - nb - 1
        if 0 <= t < len(swaps):
            swaps[t](0)
            swaps[t](1)
        if s == n + LAG - 2:
            relay(*events[0])
    for k in range(quarter):
        swap_prior(0, k)
        swap_prior(1, k)

    lane = lax.broadcasted_iota(jnp.int32, (SUB, LANE), 1)
    for field in (POST, PRIOR):
        packed = jnp.zeros((SUB, LANE), jnp.float32)
        for block in range(nblocks):
            packed = jnp.where(lane == block, jnp.sum(spread[field, block], axis=1, keepdims=True), packed)
        part1[hz, field] = packed
    for i in range(1, blocks):
        send(part1.at[hz], part1.at[hz], h_send.at[i], h_recv.at[hz], {"mem": m, "hz": lax.rem(hz + i, blocks)})

    for event in events[1:cut1]:
        relay(*event)
    for i in range(1, blocks):
        src = lax.rem(hz + i, blocks)
        arrive(part1.at[src], h_send.at[i], h_recv.at[src])
    for field in (POST, PRIOR):
        v = part1[0, field]
        for i in range(1, blocks):
            v = v + part1[i, field]
        part2[m, field] = v
    for i in range(1, members):
        send(part2.at[m], part2.at[m], m_send.at[i], m_recv.at[m], {"mem": lax.rem(m + i, members), "hz": hz})
    for event in events[cut1:cut2]:
        relay(*event)
    for i in range(1, members):
        src = lax.rem(m + i, members)
        arrive(part2.at[src], m_send.at[i], m_recv.at[src])
    spreads = []
    for field in (POST, PRIOR):
        v = part2[0, field]
        for i in range(1, members):
            v = v + part2[i, field]
        spreads.append(v)
    sub = lax.broadcasted_iota(jnp.int32, (SUB, LANE), 0)
    relax = jnp.zeros((SUB, LANE), jnp.float32)
    for level in range(levels):
        relax = jnp.where((sub == level % SUB) & (lane == level // SUB), relax_ref[level], relax)
    factor = relax * (jnp.sqrt((spreads[PRIOR] + eps) / (spreads[POST] + eps)) - 1.0) + 1.0
    for block in range(nblocks):
        zero[block] = jnp.broadcast_to(
            jnp.sum(jnp.where(lane == block, factor, 0.0), axis=1, keepdims=True), (SUB, LANE))
    control_load.wait()

    outs = []

    def finish(block, h):
        f = zero[block]
        c, p, t, o = (r.at[rows(block), cols(h)] for r in (control, x.at[POST], total, out))
        for j in range(half // LANE):
            at = slice(j * LANE, (j + 1) * LANE)
            o[:, at] = c[:, at] + f * (p[:, at] - t[:, at] / members)
        copy = pltpu.make_async_copy(o, out_hbm.at[0, rows(block), cols(h)], out_sem.at[block, h])
        copy.start()
        outs.append(copy)

    for i, (d, h, k) in enumerate(events):
        if i >= cut2:
            relay(d, h, k)
        if h is None:
            finish(d * quarter + k, y)
        else:
            finish(2 * quarter + d * quarter + k, h)
    for k in range(quarter):
        for d in (near, far):
            i = d * quarter + k
            arrive(total.at[rows(i), cols(other)], gy_send.at[i], gy_recv.at[i])
            finish(i, other)
    for cond, copy in pending:
        if cond is None:
            copy.wait_send()
        else:
            pl.when(cond)(copy.wait_send)
    for copy in outs:
        copy.wait()


def solution(mesh):
    members, blocks = mesh.shape["mem"], mesh.shape["hz"]

    def on_device(prior, posterior, control, relax, ocean):
        levels, columns = control.shape
        half, nblocks = columns // 2, levels // SUB
        a, q = nblocks // 2, nblocks // 4
        vmem = lambda *shape: pltpu.VMEM(shape, jnp.float32)
        dma = lambda *shape: pltpu.SemaphoreType.DMA(shape)
        hbm = pl.BlockSpec(memory_space=pl.ANY)
        return pl.pallas_call(
            functools.partial(kernel, members, blocks),
            out_shape=jax.ShapeDtypeStruct(posterior.shape, jnp.float32),
            in_specs=[hbm, hbm, hbm, pl.BlockSpec(memory_space=pltpu.SMEM), pl.BlockSpec(memory_space=pltpu.VMEM)],
            out_specs=hbm,
            scratch_shapes=[
                vmem(2, levels, columns), vmem(levels, columns), vmem(SUB, columns), vmem(levels, columns),
                vmem(levels, columns), vmem(2, a, SUB, half), vmem(2, a, SUB, half), vmem(2, a, SUB, half),
                vmem(2, a, 2, SUB, half), vmem(2, a, 2, SUB, half), vmem(a, 2, SUB, half), vmem(a, SUB, half),
                vmem(2, nblocks, SUB, LANE), vmem(blocks, 2, SUB, LANE), vmem(members, 2, SUB, LANE),
                vmem(nblocks, SUB, LANE),
                dma(2, nblocks), pltpu.SemaphoreType.DMA, dma(nblocks, 2),
                dma(2, a), dma(2, a), dma(2, a), dma(2, a), dma(2, a, 2), dma(2, a, 2), dma(a, 2), dma(a, 2), dma(a), dma(a),
                dma(a), dma(a), dma(a), dma(a), dma(a, 2), dma(a, 2), dma(blocks), dma(blocks), dma(members), dma(members),
            ],
            compiler_params=pltpu.CompilerParams(
                collective_id=0, has_side_effects=True, vmem_limit_bytes=60 * 2**20
            ),
        )(prior, posterior, control, relax, ocean.reshape(1, columns))

    return jax.shard_map(
        on_device,
        mesh=mesh,
        in_specs=(P("mem", None, "hz"), P("mem", None, "hz"), P(None, "hz"), P(), P("hz")),
        out_specs=P("mem", None, "hz"),
        check_vma=False,
    )
```
